32 devices in a mesh: field: 2 (over core), dom: 16 (over z, y, x).
Axes of the slice: x: 2, y: 2, z: 4, core: 2. Of those that a mesh axis runs over, the one named last changes fastest.
Arguments:
- modes: float32 [2, 40, 131072], P('field', None, 'dom'), may hold values from -6 to 6
- previous: float32 [2, 40, 131072], P('field', None, 'dom'), may hold values from -6 to 6
- kinds: int32 [2, 3, 256], P('field'), may hold values from 0 to 3
- scales: float32 [2, 3, 256], P('field'), may hold values from 0.5 to 4
- tables: bfloat16 [2, 3, 4, 512, 512], P('field'), may hold values from -2 to 6, as said below
- wet_rows: int32 [2, 49152], P('field', 'dom'), may hold values from 0 to 8191, as said below
- wet_counts: int32 [16], P('dom'), may hold values from 768 to 3072, as said below
- coupling: float32 [49152], P('dom'), may hold values from -6 to 6
Outputs:
- basis: float32 [2, 120, 131072], P('field', None, 'dom')
- projected: float32 [120, 120], replicated
The draws below stay inside these ranges and needn't reach their ends.
Inputs may be any that keep to these rules, and one draw needn't show every extreme that they name: `tables`: tables of offset 0 are symmetric. `wet_rows`: within each subdomain and field the 3072 row numbers are distinct. `wet_counts`: some subdomain uses all 3072 slots.
All inputs are finite; a program needn't handle non-finite values.
Results may differ from the reference program's by a relative error of at most 0.00045.
The reference program's roundings to bfloat16 on the way count: a program that leaves them out, or rounds other values in their place, can miss the bound.
Values may be sent and summed in bfloat16 or wider, within the bound.
A program may use at most 192 MiB of HBM per device.

```python
import math
import jax
import jax.numpy as jnp
from jax import lax

MODES = 40
BS = 512
NTYPE = 4
NBR = 16
ROWS_DEV = 8192
IFACE = 3072
SUBDOMS = 16
NBLK = 256
NF = 131072


def draw_tables(key, part):
    first, second = jax.random.split(key, 2)
    shape = (2, 3, NTYPE, BS, BS)
    noise = jnp.clip(jax.random.normal(first, shape, jnp.float32), -4.0, 4.0)
    noise = noise / jnp.sqrt(jnp.float32(BS))
    symmetric = (noise + jnp.swapaxes(noise, -1, -2)) * 0.70710678
    diagonal = jax.random.uniform(second, (2, 3, NTYPE, BS), jnp.float32, 2.0, 4.0)
    identity = jnp.eye(BS, dtype=jnp.float32)
    centre = symmetric + identity * diagonal[..., None]
    which = jnp.arange(3)[None, :, None, None, None] == 0
    return jnp.where(which, centre, noise).astype(jnp.bfloat16)


def draw_wet_rows(key, part):
    keys = jax.random.split(jax.random.fold_in(key, 11), 2 * SUBDOMS)
    chosen = jax.vmap(lambda single: jax.random.permutation(single, ROWS_DEV)[:IFACE])(keys)
    return chosen.reshape(2, SUBDOMS * IFACE).astype(jnp.int32)


def draw_wet_counts(key, part):
    first, second = jax.random.split(jax.random.fold_in(key, 23), 2)
    counts = jax.random.randint(first, (SUBDOMS,), IFACE // 4, IFACE + 1)
    fullest = jax.random.randint(second, (), 0, SUBDOMS)
    return jnp.where(jnp.arange(SUBDOMS) == fullest, IFACE, counts).astype(jnp.int32)


def place_ends(array, own_key, smallest, high):
    longest = array.shape.index(max(array.shape))
    spots = []
    for shift in (0, 1):
        where = [jax.random.randint(jax.random.fold_in(own_key, axis), (), 0, length) for axis, length in enumerate(array.shape)]
        where[longest] = (where[longest] + shift) % array.shape[longest]
        spots.append(tuple(where))
    return array.at[spots[0]].set(smallest).at[spots[1]].set(high)


def block_scale(own_key, extent, cuts, smallest, top_value):
    def one(position, parts):
        heights = jax.random.uniform(jax.random.fold_in(jax.random.fold_in(own_key, 6), position), (parts,), jnp.float32, smallest / len(cuts), top_value / len(cuts))
        return jnp.repeat(jnp.exp(heights), extent[position] // parts).reshape((-1,) + (1,) * (len(extent) - position - 1))

    factor_of = one(*cuts[0])
    for cut in cuts[1:]:
        factor_of = factor_of * one(*cut)
    return factor_of


def bell_draw(own_key, shape, deviation, limit, cuts=(), kind=jnp.bfloat16):
    values = jax.random.normal(own_key, shape, jnp.float32) * deviation
    if len(cuts) > 0:
        values = block_scale(own_key, shape, cuts, -0.22, 0.18) * values
    return jnp.clip(values, min=-limit, max=limit).astype(kind)


def setup_inputs(seed: int = 0) -> dict:
    splits = jax.random.split(jax.random.key(seed), 9)
    return {
        "modes": bell_draw(splits[0], (2, MODES, NF), 1.0, 6.0, ((0, 2), (2, 16)), jnp.float32),
        "previous": bell_draw(splits[1], (2, MODES, NF), 1.0, 6.0, ((0, 2), (2, 16)), jnp.float32),
        "kinds": place_ends(jax.random.randint(splits[2], (2, 3, NBLK), 0, NTYPE), jax.random.fold_in(splits[2], 1), 0, NTYPE - 1).astype(jnp.int32),
        "scales": jnp.clip(jnp.exp(math.log(4.0) - 2.0794415 * jax.random.uniform(splits[3], (2, 3, NBLK), jnp.float32) ** block_scale(splits[3], (2, 3, NBLK), ((0, 2),), -0.2, 0.2)), 0.5, 4.0),
        "tables": draw_tables(jax.random.fold_in(splits[8], 71), 0),
        "wet_rows": draw_wet_rows(jax.random.fold_in(splits[8], 71), 0),
        "wet_counts": draw_wet_counts(jax.random.fold_in(splits[8], 71), 0),
        "coupling": bell_draw(splits[7], (SUBDOMS * IFACE,), 1.0, 6.0, ((0, 16),), jnp.float32),
    }


def block_product(window, kinds, scales, tables):
    columns = window.shape[0]
    blocks = window.reshape(columns, NBR + 4, BS).astype(jnp.float32)
    centre = tables[0][kinds[0, 2:]].astype(jnp.float32)
    result = scales[0, 2:][None, :, None] * jnp.einsum('cni,nji->cnj', blocks[:, 2:NBR + 2], centre)
    for offset in (1, 2):
        ahead = tables[offset][kinds[offset, 2:]].astype(jnp.float32)
        result = result + scales[offset, 2:][None, :, None] * jnp.einsum('cni,nji->cnj', blocks[:, 2 + offset:NBR + 2 + offset], ahead)
        behind = tables[offset][kinds[offset, 2 - offset:NBR + 2 - offset]].astype(jnp.float32)
        result = result + scales[offset, 2 - offset:NBR + 2 - offset][None, :, None] * jnp.einsum('cni,nij->cnj', blocks[:, 2 - offset:NBR + 2 - offset], behind)
    return result.reshape(columns, NBR * BS)

def field_blocks(vectors, kinds, scales, tables):
    columns = vectors.shape[0]
    padded = jnp.pad(vectors.astype(jnp.bfloat16), ((0, 0), (2 * BS, 2 * BS)))
    kinds_pad = jnp.pad(kinds, ((0, 0), (2, 0)))
    scales_pad = jnp.pad(scales, ((0, 0), (2, 0)))

    def one_domain(domain):
        window = lax.dynamic_slice_in_dim(padded, domain * ROWS_DEV, ROWS_DEV + 4 * BS, 1)
        local_kinds = lax.dynamic_slice_in_dim(kinds_pad, domain * NBR, NBR + 2, 1)
        local_scales = lax.dynamic_slice_in_dim(scales_pad, domain * NBR, NBR + 2, 1)
        return block_product(window, local_kinds, local_scales, tables)
    pieces = lax.map(one_domain, jnp.arange(SUBDOMS, dtype=jnp.int32))
    return jnp.transpose(pieces, (1, 0, 2)).reshape(columns, SUBDOMS * ROWS_DEV)

def operator(vectors, kinds, scales, tables, global_rows, weights):
    images = [field_blocks(vectors[field_id], kinds[field_id], scales[field_id], tables[field_id]) for field_id in range(2)]
    coupled = []
    for field_id in range(2):
        other = 1 - field_id
        values = vectors[other][:, global_rows[other]] * weights[None, :]
        coupled.append(images[field_id].at[:, global_rows[field_id]].add(values))
    return jnp.stack(coupled)

def reference(modes, previous, kinds, scales, tables, wet_rows, wet_counts, coupling):
    highest = lax.Precision.HIGHEST
    offsets = jnp.arange(SUBDOMS, dtype=jnp.int32)[:, None] * ROWS_DEV
    global_rows = (wet_rows.reshape(2, SUBDOMS, IFACE) + offsets[None]).reshape(2, SUBDOMS * IFACE)
    used = jnp.arange(IFACE, dtype=jnp.int32)[None, :] < wet_counts[:, None]
    weights = jnp.where(used, coupling.reshape(SUBDOMS, IFACE), jnp.float32(0.0)).reshape(SUBDOMS * IFACE)
    image_x = operator(modes, kinds, scales, tables, global_rows, weights)
    quotient = jnp.sum(modes * image_x, axis=(0, 2)) / jnp.sum(modes * modes, axis=(0, 2))
    diag_table = jnp.diagonal(tables[:, 0], axis1=-2, axis2=-1).astype(jnp.float32)
    jacobi = jnp.stack([(scales[field_id, 0][:, None] * diag_table[field_id][kinds[field_id, 0]]).reshape(SUBDOMS * ROWS_DEV) for field_id in range(2)])
    residual_dir = (image_x - modes * quotient[None, :, None]) / jacobi[:, None, :]
    image_wp = operator(jnp.concatenate([residual_dir, previous], axis=1), kinds, scales, tables, global_rows, weights)
    search = jnp.concatenate([modes, residual_dir, previous], axis=1)
    image_all = jnp.concatenate([image_x, image_wp], axis=1)
    ndof = 2.0 * SUBDOMS * ROWS_DEV
    gram_b = (jnp.dot(search[0], search[0].T, precision=highest) + jnp.dot(search[1], search[1].T, precision=highest)) / ndof
    raw = jnp.dot(search[0], image_all[0].T, precision=highest) + jnp.dot(search[1], image_all[1].T, precision=highest)
    gram_a = (raw + raw.T) / (2.0 * ndof)
    chol = jnp.linalg.cholesky(gram_b)
    leading = jax.scipy.linalg.solve_triangular(chol, gram_a, lower=True)
    projected = jax.scipy.linalg.solve_triangular(chol, leading.T, lower=True)
    basis = jnp.stack([jax.scipy.linalg.solve_triangular(chol, search[field_id], lower=True) for field_id in range(2)])
    return (basis, projected)
```

```python
import functools

import jax
import jax.numpy as jnp
from jax import lax
from jax.experimental import pallas as pl
from jax.experimental.pallas import tpu as pltpu
from jax.sharding import PartitionSpec as P

BS = 512


def for_sending(shard):
    return jax.tree.map(lambda a: a.astype(jnp.bfloat16) if a.dtype == jnp.float32 else a, shard)


def swapped(shard, axis, apart):
    return lax.ppermute(shard, axis, [(i, i ^ 1 << apart) for i in range(lax.axis_size(axis))])


def halos(cells, axis, dim, width):
    count = lax.axis_size(axis)
    ends = count - 1
    head = lax.slice_in_dim(cells, 0, width, axis=dim)
    tail = lax.slice_in_dim(cells, cells.shape[dim] - width, cells.shape[dim], axis=dim)
    return (
        lax.ppermute(tail, axis, [(i, i + 1) for i in range(ends)]),
        lax.ppermute(head, axis, [(i + 1, i) for i in range(ends)]),
    )


def doubling_kernel(bits, x_ref, o_ref, held, landed, send_sem, recv_sem):
    field = lax.axis_index("field")
    dom = lax.axis_index("dom")
    partners = [(1 - field, dom)]
    for bit in range(bits):
        step = 1 << bit
        partners.append((field, dom + (1 - 2 * ((dom // step) % 2)) * step))
    barrier = pltpu.get_barrier_semaphore()
    for partner in partners:
        pl.semaphore_signal(
            barrier, inc=1, device_id=partner, device_id_type=pl.DeviceIdType.MESH
        )
    held[0] = x_ref[...]
    pl.semaphore_wait(barrier, len(partners))
    for step, partner in enumerate(partners):
        copy = pltpu.make_async_remote_copy(
            src_ref=held.at[step],
            dst_ref=landed.at[step],
            send_sem=send_sem.at[step],
            recv_sem=recv_sem.at[step],
            device_id=partner,
            device_id_type=pl.DeviceIdType.MESH,
        )
        copy.start()
        copy.wait()
        total = held[step] + landed[step]
        if step + 1 < len(partners):
            held[step + 1] = total
        else:
            o_ref[...] = total


def summed_everywhere(x, collective_id):
    bits = (lax.axis_size("dom") - 1).bit_length()
    steps = bits + 1
    return pl.pallas_call(
        functools.partial(doubling_kernel, bits),
        out_shape=jax.ShapeDtypeStruct(x.shape, x.dtype),
        in_specs=[pl.BlockSpec(memory_space=pltpu.VMEM)],
        out_specs=pl.BlockSpec(memory_space=pltpu.VMEM),
        scratch_shapes=[
            pltpu.VMEM((steps,) + x.shape, x.dtype),
            pltpu.VMEM((steps,) + x.shape, x.dtype),
            pltpu.SemaphoreType.DMA((steps,)),
            pltpu.SemaphoreType.DMA((steps,)),
        ],
        compiler_params=pltpu.CompilerParams(
            collective_id=collective_id, has_side_effects=True
        ),
    )(x)


NN = (((1,), (0,)), ((), ()))
NT = (((1,), (1,)), ((), ()))


def stencil_kernel(kinds, scales, x_ref, before, after, tables, o_ref, window):
    nbr = x_ref.shape[1] // BS
    wide = x_ref.shape[1]
    window[:, : 2 * BS] = before[...]
    window[:, 2 * BS : 2 * BS + wide] = x_ref[...].astype(jnp.bfloat16)
    window[:, 2 * BS + wide :] = after[...]

    def term(n, shift, offset, at, dims):
        block = window[:, pl.ds(pl.multiple_of((n + 2 + shift) * BS, BS), BS)]
        product = lax.dot_general(
            block, tables[offset, kinds[offset, at]], dims, preferred_element_type=jnp.float32
        )
        return scales[offset, at] * product

    def step(n, carry):
        total = term(n, 0, 0, n + 2, NN)
        for offset in (1, 2):
            total = total + term(n, offset, offset, n + 2, NT)
            total = total + term(n, -offset, offset, n + 2 - offset, NN)
        o_ref[:, pl.ds(pl.multiple_of(n * BS, BS), BS)] = total
        return carry

    lax.fori_loop(0, nbr, step, 0)


def block_product(vectors, sides, kinds, scales, tables):
    columns, wide = vectors.shape
    smem = pl.BlockSpec(memory_space=pltpu.SMEM)
    vmem = pl.BlockSpec(memory_space=pltpu.VMEM)
    return pl.pallas_call(
        stencil_kernel,
        out_shape=jax.ShapeDtypeStruct((columns, wide), jnp.float32),
        in_specs=[smem, smem, vmem, vmem, vmem, vmem],
        out_specs=vmem,
        scratch_shapes=[pltpu.VMEM((columns, wide + 4 * BS), jnp.bfloat16)],
        cost_estimate=pl.CostEstimate(
            flops=10 * columns * wide * BS, bytes_accessed=16 * columns * wide, transcendentals=0
        ),
        compiler_params=pltpu.CompilerParams(vmem_limit_bytes=30 * 1024 * 1024),
    )(kinds, scales, vectors, *sides, tables)


def operate(vectors, kinds, scales, tables, rows, weights):
    sides = halos(vectors.astype(jnp.bfloat16), "dom", 1, 2 * BS)
    values = jnp.take(vectors, rows, axis=1) * weights[None, :]
    received = swapped(for_sending(values), "field", 0).astype(values.dtype)
    images = block_product(vectors, sides, kinds, scales, tables)
    return images.at[:, rows].add(received)


def shards(modes, previous, kinds, scales, tables, wet_rows, wet_counts, coupling):
    high = lax.Precision.HIGH
    domain = lax.axis_index("dom")
    vec_modes = modes[0]
    vec_prev = previous[0]
    columns, wide = vec_modes.shape
    nbr = wide // BS
    field_tables = tables[0]
    types = field_tables.shape[1]
    kinds_pad = jnp.pad(kinds[0], ((0, 0), (2, 0)))
    scales_pad = jnp.pad(scales[0], ((0, 0), (2, 0)))
    local_kinds = lax.dynamic_slice_in_dim(kinds_pad, domain * nbr, nbr + 2, 1)
    local_scales = lax.dynamic_slice_in_dim(scales_pad, domain * nbr, nbr + 2, 1)
    rows = wet_rows[0]
    slots = coupling.shape[0]
    used = jnp.arange(slots, dtype=jnp.int32) < wet_counts[0]
    weights = jnp.where(used, coupling, jnp.float32(0.0))
    operands = (local_kinds, local_scales, field_tables, rows, weights)
    first_pair = jnp.concatenate([vec_modes, vec_prev], axis=0)
    image_pair = operate(first_pair, *operands)
    image_x, image_p = image_pair[:columns], image_pair[columns:]
    partial_sums = jnp.stack(
        [jnp.sum(vec_modes * vec_modes, axis=1), jnp.sum(vec_modes * image_x, axis=1)]
    )
    sums = summed_everywhere(jnp.pad(partial_sums, ((0, 6), (0, 128 - columns))), 1)
    quotient = sums[1, :columns] / sums[0, :columns]
    eye = jnp.eye(BS, dtype=jnp.bool_)
    diag_table = jnp.sum(
        jnp.where(eye[None], field_tables[0].astype(jnp.float32), jnp.float32(0.0)), axis=1
    )
    row_diag = jnp.zeros((nbr, BS), jnp.float32)
    for type_id in range(types):
        row_diag = jnp.where(
            (local_kinds[0, 2:] == type_id)[:, None], diag_table[type_id][None, :], row_diag
        )
    jacobi = (local_scales[0, 2:][:, None] * row_diag).reshape(wide)
    residual_dir = (image_x - vec_modes * quotient[:, None]) / jacobi[None, :]
    image_r = operate(residual_dir, *operands)
    search = jnp.concatenate([vec_modes, residual_dir, vec_prev], axis=0)
    image_all = jnp.concatenate([image_x, image_r, image_p], axis=0)
    ndof = 2.0 * lax.axis_size("dom") * wide
    part_b = jnp.dot(search, search.T, precision=high)
    part_a = jnp.dot(search, image_all.T, precision=high)
    part_a = part_a + part_a.T
    size = 3 * columns
    row = lax.broadcasted_iota(jnp.int32, (size, size + 8), 0)
    col = lax.broadcasted_iota(jnp.int32, (size, size + 8), 1)
    packed = jnp.where(
        col <= row,
        jnp.pad(part_b, ((0, 0), (0, 8))),
        jnp.pad(part_a, ((0, 0), (1, 7))),
    )
    packed = summed_everywhere(packed, 2)
    low = jnp.where(col <= row, packed, 0.0)[:, :size]
    high_part = packed[:, 1 : size + 1]
    square_row, square_col = row[:, :size], col[:, :size]
    gram_b = jnp.where(square_col <= square_row, low, low.T) / ndof
    gram_a = jnp.where(square_col >= square_row, high_part, high_part.T) / (2.0 * ndof)
    chol = jnp.linalg.cholesky(gram_b, symmetrize_input=False)
    leading = jax.scipy.linalg.solve_triangular(chol, gram_a, lower=True)
    projected = jax.scipy.linalg.solve_triangular(chol, leading.T, lower=True)
    basis = jax.scipy.linalg.solve_triangular(chol, search, lower=True)
    return (basis[None], projected)


def solution(mesh):
    return jax.shard_map(
        shards,
        mesh=mesh,
        in_specs=(
            P("field", None, "dom"),
            P("field", None, "dom"),
            P("field", None, None),
            P("field", None, None),
            P("field", None, None, None, None),
            P("field", "dom"),
            P("dom"),
            P("dom"),
        ),
        out_specs=(P("field", None, "dom"), P()),
        check_vma=False,
    )
```

```python
import functools

import jax
import jax.numpy as jnp
from jax import lax
from jax.experimental import pallas as pl
from jax.experimental.pallas import tpu as pltpu
from jax.sharding import PartitionSpec as P

BS = 512
LANES = 128
SHIFT = 16


def swapped(shard, axis, apart):
    return lax.ppermute(shard, axis, [(i, i ^ 1 << apart) for i in range(lax.axis_size(axis))])


def halos(cells, axis, dim, width):
    count = lax.axis_size(axis)
    ends = count - 1
    head = lax.slice_in_dim(cells, 0, width, axis=dim)
    tail = lax.slice_in_dim(cells, cells.shape[dim] - width, cells.shape[dim], axis=dim)
    return (
        lax.ppermute(tail, axis, [(i, i + 1) for i in range(ends)]),
        lax.ppermute(head, axis, [(i + 1, i) for i in range(ends)]),
    )


def doubling_kernel(bits, x_ref, o_ref, held, landed, send_sem, recv_sem):
    field = lax.axis_index("field")
    dom = lax.axis_index("dom")
    partners = [(1 - field, dom)]
    for bit in range(bits):
        step = 1 << bit
        partners.append((field, dom + (1 - 2 * ((dom // step) % 2)) * step))
    barrier = pltpu.get_barrier_semaphore()
    for partner in partners:
        pl.semaphore_signal(
            barrier, inc=1, device_id=partner, device_id_type=pl.DeviceIdType.MESH
        )
    held[0] = x_ref[...]
    pl.semaphore_wait(barrier, len(partners))
    for step, partner in enumerate(partners):
        copy = pltpu.make_async_remote_copy(
            src_ref=held.at[step],
            dst_ref=landed.at[step],
            send_sem=send_sem.at[step],
            recv_sem=recv_sem.at[step],
            device_id=partner,
            device_id_type=pl.DeviceIdType.MESH,
        )
        copy.start()
        copy.wait()
        total = held[step] + landed[step]
        if step + 1 < len(partners):
            held[step + 1] = total
        else:
            o_ref[...] = total


def summed_everywhere(x, collective_id):
    bits = (lax.axis_size("dom") - 1).bit_length()
    steps = bits + 1
    return pl.pallas_call(
        functools.partial(doubling_kernel, bits),
        out_shape=jax.ShapeDtypeStruct(x.shape, x.dtype),
        in_specs=[pl.BlockSpec(memory_space=pltpu.VMEM)],
        out_specs=pl.BlockSpec(memory_space=pltpu.VMEM),
        scratch_shapes=[
            pltpu.VMEM((steps,) + x.shape, x.dtype),
            pltpu.VMEM((steps,) + x.shape, x.dtype),
            pltpu.SemaphoreType.DMA((steps,)),
            pltpu.SemaphoreType.DMA((steps,)),
        ],
        compiler_params=pltpu.CompilerParams(
            collective_id=collective_id, has_side_effects=True
        ),
    )(x)


NN = (((1,), (0,)), ((), ()))
NT = (((1,), (1,)), ((), ()))


def operator_kernel(
    kinds, scales, places, weights, x_ref, before, after, other, tables, o_ref, window, rows_in, rows_out
):
    columns, wide = x_ref.shape
    nbr = wide // BS
    share = places.shape[0] // nbr
    window[:, : 2 * BS] = before[...]
    window[:, 2 * BS : 2 * BS + wide] = x_ref[...].astype(jnp.bfloat16)
    window[:, 2 * BS + wide :] = after[...]
    blank = jnp.zeros((LANES - columns, LANES), jnp.float32)

    def turn_in(tile, carry):
        span = pl.ds(pl.multiple_of(tile * LANES, LANES), LANES)
        cell = jnp.concatenate([other[:, span].astype(jnp.float32), blank], axis=0)
        rows_in[span, :] = cell.T
        rows_out[span, :] = jnp.zeros((LANES, LANES), jnp.float32)
        return carry

    lax.fori_loop(0, wide // LANES, turn_in, 0, unroll=2)

    def term(n, shift, offset, at, dims):
        block = window[:, pl.ds(pl.multiple_of((n + 2 + shift) * BS, BS), BS)]
        product = lax.dot_general(
            block, tables[offset, kinds[offset, at]], dims, preferred_element_type=jnp.float32
        )
        return scales[offset, at] * product

    def step(n, carry):
        total = term(n, 0, 0, n + 2, NN)
        for offset in (1, 2):
            total = total + term(n, offset, offset, n + 2, NT)
            total = total + term(n, -offset, offset, n + 2 - offset, NN)
        o_ref[:, pl.ds(pl.multiple_of(n * BS, BS), BS)] = total
        for slot in range(share):
            place = places[n * share + slot]
            source = lax.shift_right_logical(place, SHIFT)
            target = lax.bitwise_and(place, (1 << SHIFT) - 1)
            rows_out[pl.ds(target, 1), :] = rows_in[pl.ds(source, 1), :] * weights[n * share + slot]
        return carry

    lax.fori_loop(0, nbr, step, 0)

    def turn_out(tile, carry):
        span = pl.ds(pl.multiple_of(tile * LANES, LANES), LANES)
        o_ref[:, span] = o_ref[:, span] + rows_out[span, :].T[:columns]
        return carry

    lax.fori_loop(0, wide // LANES, turn_out, 0, unroll=2)


def operate(vectors, kinds, scales, tables, places, weights):
    columns, wide = vectors.shape
    rounded = vectors.astype(jnp.bfloat16)
    other = swapped(rounded, "field", 0)
    before, after = halos(rounded, "dom", 1, 2 * BS)
    smem = pl.BlockSpec(memory_space=pltpu.SMEM)
    vmem = pl.BlockSpec(memory_space=pltpu.VMEM)
    return pl.pallas_call(
        operator_kernel,
        out_shape=jax.ShapeDtypeStruct((columns, wide), jnp.float32),
        in_specs=[smem, smem, smem, smem, vmem, vmem, vmem, vmem, vmem],
        out_specs=vmem,
        scratch_shapes=[
            pltpu.VMEM((columns, wide + 4 * BS), jnp.bfloat16),
            pltpu.VMEM((wide, LANES), jnp.float32),
            pltpu.VMEM((wide, LANES), jnp.float32),
        ],
        cost_estimate=pl.CostEstimate(
            flops=10 * columns * wide * BS, bytes_accessed=16 * columns * wide, transcendentals=0
        ),
        compiler_params=pltpu.CompilerParams(vmem_limit_bytes=40 * 1024 * 1024),
    )(kinds, scales, places, weights, vectors, before, after, other, tables)


def shards(modes, previous, kinds, scales, tables, wet_rows, wet_counts, coupling):
    high = lax.Precision.HIGH
    domain = lax.axis_index("dom")
    vec_modes = modes[0]
    vec_prev = previous[0]
    columns, wide = vec_modes.shape
    nbr = wide // BS
    field_tables = tables[0]
    types = field_tables.shape[1]
    kinds_pad = jnp.pad(kinds[0], ((0, 0), (2, 0)))
    scales_pad = jnp.pad(scales[0], ((0, 0), (2, 0)))
    local_kinds = lax.dynamic_slice_in_dim(kinds_pad, domain * nbr, nbr + 2, 1)
    local_scales = lax.dynamic_slice_in_dim(scales_pad, domain * nbr, nbr + 2, 1)
    rows = wet_rows[0]
    slots = coupling.shape[0]
    used = jnp.arange(slots, dtype=jnp.int32) < wet_counts[0]
    weights = jnp.where(used, coupling, jnp.float32(0.0))
    places = (swapped(rows, "field", 0) << SHIFT) | rows
    operands = (local_kinds, local_scales, field_tables, places, weights)
    first_pair = jnp.concatenate([vec_modes, vec_prev], axis=0)
    image_pair = operate(first_pair, *operands)
    image_x, image_p = image_pair[:columns], image_pair[columns:]
    partial_sums = jnp.stack(
        [jnp.sum(vec_modes * vec_modes, axis=1), jnp.sum(vec_modes * image_x, axis=1)]
    )
    sums = summed_everywhere(jnp.pad(partial_sums, ((0, 6), (0, 128 - columns))), 1)
    quotient = sums[1, :columns] / sums[0, :columns]
    eye = jnp.eye(BS, dtype=jnp.bool_)
    diag_table = jnp.sum(
        jnp.where(eye[None], field_tables[0].astype(jnp.float32), jnp.float32(0.0)), axis=1
    )
    row_diag = jnp.zeros((nbr, BS), jnp.float32)
    for type_id in range(types):
        row_diag = jnp.where(
            (local_kinds[0, 2:] == type_id)[:, None], diag_table[type_id][None, :], row_diag
        )
    jacobi = (local_scales[0, 2:][:, None] * row_diag).reshape(wide)
    residual_dir = (image_x - vec_modes * quotient[:, None]) / jacobi[None, :]
    image_r = operate(residual_dir, *operands)
    search = jnp.concatenate([vec_modes, residual_dir, vec_prev], axis=0)
    image_all = jnp.concatenate([image_x, image_r, image_p], axis=0)
    ndof = 2.0 * lax.axis_size("dom") * wide
    part_b = jnp.dot(search, search.T, precision=high)
    part_a = jnp.dot(search, image_all.T, precision=high)
    part_a = part_a + part_a.T
    size = 3 * columns
    row = lax.broadcasted_iota(jnp.int32, (size, size + 8), 0)
    col = lax.broadcasted_iota(jnp.int32, (size, size + 8), 1)
    packed = jnp.where(
        col <= row,
        jnp.pad(part_b, ((0, 0), (0, 8))),
        jnp.pad(part_a, ((0, 0), (1, 7))),
    )
    packed = summed_everywhere(packed, 2)
    low = jnp.where(col <= row, packed, 0.0)[:, :size]
    high_part = packed[:, 1 : size + 1]
    square_row, square_col = row[:, :size], col[:, :size]
    gram_b = jnp.where(square_col <= square_row, low, low.T) / ndof
    gram_a = jnp.where(square_col >= square_row, high_part, high_part.T) / (2.0 * ndof)
    chol = jnp.linalg.cholesky(gram_b, symmetrize_input=False)
    leading = jax.scipy.linalg.solve_triangular(chol, gram_a, lower=True)
    projected = jax.scipy.linalg.solve_triangular(chol, leading.T, lower=True)
    basis = jax.scipy.linalg.solve_triangular(chol, search, lower=True)
    return (basis[None], projected)


def solution(mesh):
    return jax.shard_map(
        shards,
        mesh=mesh,
        in_specs=(
            P("field", None, "dom"),
            P("field", None, "dom"),
            P("field", None, None),
            P("field", None, None),
            P("field", None, None, None, None),
            P("field", "dom"),
            P("dom"),
            P("dom"),
        ),
        out_specs=(P("field", None, "dom"), P()),
        check_vma=False,
    )
```

```python
import functools

import jax
import jax.numpy as jnp
from jax import lax
from jax.experimental import pallas as pl
from jax.experimental.pallas import tpu as pltpu
from jax.sharding import PartitionSpec as P

BS = 512
LANES = 128
SHIFT = 16


def swapped(shard, axis, apart):
    return lax.ppermute(shard, axis, [(i, i ^ 1 << apart) for i in range(lax.axis_size(axis))])


def halos(cells, axis, dim, width):
    count = lax.axis_size(axis)
    ends = count - 1
    head = lax.slice_in_dim(cells, 0, width, axis=dim)
    tail = lax.slice_in_dim(cells, cells.shape[dim] - width, cells.shape[dim], axis=dim)
    return (
        lax.ppermute(tail, axis, [(i, i + 1) for i in range(ends)]),
        lax.ppermute(head, axis, [(i + 1, i) for i in range(ends)]),
    )


def sum_kernel(rounds, split, x_ref, o_ref, held, landed, across, send_sem, recv_sem, side_send, side_recv):
    field = lax.axis_index("field")
    dom = lax.axis_index("dom")
    groups = []
    for step, members in rounds:
        low = (1 - 2 * ((dom // step) % 2)) * step
        high = (1 - 2 * ((dom // (2 * step)) % 2)) * 2 * step
        groups.append([dom + (e % 2) * low + (e // 2) * high for e in range(1, members)])
    barrier = pltpu.get_barrier_semaphore()
    peers = [(1 - field, dom)] + [(field, peer) for group in groups for peer in group]
    for peer in peers:
        pl.semaphore_signal(barrier, inc=1, device_id=peer, device_id_type=pl.DeviceIdType.MESH)
    pl.semaphore_wait(barrier, len(peers))

    def send(source, target, sems, peer):
        copy = pltpu.make_async_remote_copy(
            src_ref=source,
            dst_ref=target,
            send_sem=sems[0],
            recv_sem=sems[1],
            device_id=peer,
            device_id_type=pl.DeviceIdType.MESH,
        )
        copy.start()
        return copy

    mine, theirs = (field, 1 - field) if split else (0, 0)
    copy = send(
        x_ref.at[theirs], across.at[0], (side_send.at[0], side_recv.at[0]), (1 - field, dom)
    )
    copy.wait()
    total = x_ref[mine] + across[0]
    for turn, group in enumerate(groups):
        held[turn] = total
        copies = [
            send(
                held.at[turn],
                landed.at[turn, e],
                (send_sem.at[turn, e], recv_sem.at[turn, e]),
                (field, peer),
            )
            for e, peer in enumerate(group)
        ]
        for copy in copies:
            copy.wait()
        total = total + landed[turn, 0]
        if len(group) == 3:
            total = total + (landed[turn, 1] + landed[turn, 2])
    o_ref[mine] = total
    if split:
        held[len(groups)] = total
        copy = send(
            held.at[len(groups)],
            across.at[1],
            (side_send.at[1], side_recv.at[1]),
            (1 - field, dom),
        )
        copy.wait()
        o_ref[theirs] = across[1]


def summed_everywhere(x, collective_id):
    bits = (lax.axis_size("dom") - 1).bit_length()
    rounds = [(1 << bit, 4 if bit + 1 < bits else 2) for bit in range(0, bits, 2)]
    cell = x.shape[1:]
    slots = len(rounds)
    return pl.pallas_call(
        functools.partial(sum_kernel, rounds, x.shape[0] == 2),
        out_shape=jax.ShapeDtypeStruct(x.shape, x.dtype),
        in_specs=[pl.BlockSpec(memory_space=pltpu.VMEM)],
        out_specs=pl.BlockSpec(memory_space=pltpu.VMEM),
        scratch_shapes=[
            pltpu.VMEM((slots + 1,) + cell, x.dtype),
            pltpu.VMEM((slots, 3) + cell, x.dtype),
            pltpu.VMEM((2,) + cell, x.dtype),
            pltpu.SemaphoreType.DMA((slots, 3)),
            pltpu.SemaphoreType.DMA((slots, 3)),
            pltpu.SemaphoreType.DMA((2,)),
            pltpu.SemaphoreType.DMA((2,)),
        ],
        compiler_params=pltpu.CompilerParams(
            collective_id=collective_id, has_side_effects=True
        ),
    )(x)


NN = (((1,), (0,)), ((), ()))
NT = (((1,), (1,)), ((), ()))


def operator_kernel(
    kinds, scales, places, weights, x_ref, before, after, other, tables, o_ref, window, rows_in, rows_out
):
    columns, wide = x_ref.shape
    nbr = wide // BS
    share = places.shape[0] // nbr
    window[:, : 2 * BS] = before[...]
    window[:, 2 * BS : 2 * BS + wide] = x_ref[...].astype(jnp.bfloat16)
    window[:, 2 * BS + wide :] = after[...]
    blank = jnp.zeros((LANES - columns, LANES), jnp.float32)

    def turn_in(tile, carry):
        span = pl.ds(pl.multiple_of(tile * LANES, LANES), LANES)
        cell = jnp.concatenate([other[:, span].astype(jnp.float32), blank], axis=0)
        rows_in[span, :] = cell.T
        rows_out[span, :] = jnp.zeros((LANES, LANES), jnp.float32)
        return carry

    lax.fori_loop(0, wide // LANES, turn_in, 0, unroll=16)

    def term(n, shift, offset, at, dims):
        block = window[:, pl.ds(pl.multiple_of((n + 2 + shift) * BS, BS), BS)]
        product = lax.dot_general(
            block, tables[offset, kinds[offset, at]], dims, preferred_element_type=jnp.float32
        )
        return scales[offset, at] * product

    def step(n, carry):
        total = term(n, 0, 0, n + 2, NN)
        for offset in (1, 2):
            total = total + term(n, offset, offset, n + 2, NT)
            total = total + term(n, -offset, offset, n + 2 - offset, NN)
        o_ref[:, pl.ds(pl.multiple_of(n * BS, BS), BS)] = total
        for slot in range(share):
            place = places[n * share + slot]
            source = lax.shift_right_logical(place, SHIFT)
            target = lax.bitwise_and(place, (1 << SHIFT) - 1)
            rows_out[pl.ds(target, 1), :] = rows_in[pl.ds(source, 1), :] * weights[n * share + slot]
        return carry

    lax.fori_loop(0, nbr, step, 0)

    def turn_out(tile, carry):
        span = pl.ds(pl.multiple_of(tile * LANES, LANES), LANES)
        o_ref[:, span] = o_ref[:, span] + rows_out[span, :].T[:columns]
        return carry

    lax.fori_loop(0, wide // LANES, turn_out, 0, unroll=16)


def operate(vectors, kinds, scales, tables, places, weights):
    columns, wide = vectors.shape
    rounded = vectors.astype(jnp.bfloat16)
    other = swapped(rounded, "field", 0)
    before, after = halos(rounded, "dom", 1, 2 * BS)
    smem = pl.BlockSpec(memory_space=pltpu.SMEM)
    vmem = pl.BlockSpec(memory_space=pltpu.VMEM)
    return pl.pallas_call(
        operator_kernel,
        out_shape=jax.ShapeDtypeStruct((columns, wide), jnp.float32),
        in_specs=[smem, smem, smem, smem, vmem, vmem, vmem, vmem, vmem],
        out_specs=vmem,
        scratch_shapes=[
            pltpu.VMEM((columns, wide + 4 * BS), jnp.bfloat16),
            pltpu.VMEM((wide, LANES), jnp.float32),
            pltpu.VMEM((wide, LANES), jnp.float32),
        ],
        cost_estimate=pl.CostEstimate(
            flops=10 * columns * wide * BS, bytes_accessed=16 * columns * wide, transcendentals=0
        ),
        compiler_params=pltpu.CompilerParams(vmem_limit_bytes=40 * 1024 * 1024),
    )(kinds, scales, places, weights, vectors, before, after, other, tables)


def shards(modes, previous, kinds, scales, tables, wet_rows, wet_counts, coupling):
    high = lax.Precision.HIGH
    domain = lax.axis_index("dom")
    vec_modes = modes[0]
    vec_prev = previous[0]
    columns, wide = vec_modes.shape
    nbr = wide // BS
    field_tables = tables[0]
    types = field_tables.shape[1]
    kinds_pad = jnp.pad(kinds[0], ((0, 0), (2, 0)))
    scales_pad = jnp.pad(scales[0], ((0, 0), (2, 0)))
    local_kinds = lax.dynamic_slice_in_dim(kinds_pad, domain * nbr, nbr + 2, 1)
    local_scales = lax.dynamic_slice_in_dim(scales_pad, domain * nbr, nbr + 2, 1)
    rows = wet_rows[0]
    slots = coupling.shape[0]
    used = jnp.arange(slots, dtype=jnp.int32) < wet_counts[0]
    weights = jnp.where(used, coupling, jnp.float32(0.0))
    places = (swapped(rows, "field", 0) << SHIFT) | rows
    operands = (local_kinds, local_scales, field_tables, places, weights)
    first_pair = jnp.concatenate([vec_modes, vec_prev], axis=0)
    image_pair = operate(first_pair, *operands)
    image_x, image_p = image_pair[:columns], image_pair[columns:]
    partial_sums = jnp.stack(
        [jnp.sum(vec_modes * vec_modes, axis=1), jnp.sum(vec_modes * image_x, axis=1)]
    )
    sums = summed_everywhere(jnp.pad(partial_sums, ((0, 6), (0, LANES - columns)))[None], 1)[0]
    quotient = sums[1, :columns] / sums[0, :columns]
    eye = jnp.eye(BS, dtype=jnp.bool_)
    diag_table = jnp.sum(
        jnp.where(eye[None], field_tables[0].astype(jnp.float32), jnp.float32(0.0)), axis=1
    )
    row_diag = jnp.zeros((nbr, BS), jnp.float32)
    for type_id in range(types):
        row_diag = jnp.where(
            (local_kinds[0, 2:] == type_id)[:, None], diag_table[type_id][None, :], row_diag
        )
    jacobi = (local_scales[0, 2:][:, None] * row_diag).reshape(wide)
    residual_dir = (image_x - vec_modes * quotient[:, None]) / jacobi[None, :]
    image_r = operate(residual_dir, *operands)
    search = jnp.concatenate([vec_modes, residual_dir, vec_prev], axis=0)
    image_all = jnp.concatenate([image_x, image_r, image_p], axis=0)
    ndof = 2.0 * lax.axis_size("dom") * wide
    part_b = jnp.dot(search, search.T, precision=high)
    part_a = jnp.dot(search, image_all.T, precision=high)
    part_a = part_a + part_a.T
    size = 3 * columns
    row = lax.broadcasted_iota(jnp.int32, (size, size + 8), 0)
    col = lax.broadcasted_iota(jnp.int32, (size, size + 8), 1)
    packed = jnp.where(
        col <= row,
        jnp.pad(part_b, ((0, 0), (0, 8))),
        jnp.pad(part_a, ((0, 0), (1, 7))),
    )
    half = -(-size // 16) * 8
    packed = jnp.pad(packed, ((0, 2 * half - size), (0, 0))).reshape(2, half, size + 8)
    packed = summed_everywhere(packed, 2).reshape(2 * half, size + 8)[:size]
    low = jnp.where(col <= row, packed, 0.0)[:, :size]
    high_part = packed[:, 1 : size + 1]
    square_row, square_col = row[:, :size], col[:, :size]
    gram_b = jnp.where(square_col <= square_row, low, low.T) / ndof
    gram_a = jnp.where(square_col >= square_row, high_part, high_part.T) / (2.0 * ndof)
    chol = jnp.linalg.cholesky(gram_b, symmetrize_input=False)
    leading = jax.scipy.linalg.solve_triangular(chol, gram_a, lower=True)
    projected = jax.scipy.linalg.solve_triangular(chol, leading.T, lower=True)
    basis = jax.scipy.linalg.solve_triangular(chol, search, lower=True)
    return (basis[None], projected)


def solution(mesh):
    return jax.shard_map(
        shards,
        mesh=mesh,
        in_specs=(
            P("field", None, "dom"),
            P("field", None, "dom"),
            P("field", None, None),
            P("field", None, None),
            P("field", None, None, None, None),
            P("field", "dom"),
            P("dom"),
            P("dom"),
        ),
        out_specs=(P("field", None, "dom"), P()),
        check_vma=False,
    )
```
